16 devices in a mesh: dp: 2 (over y, z), tp: 8 (over x, core).
Axes of the slice: x: 4, y: 2, z: 1, core: 2. Of those that a mesh axis runs over, the one named last changes fastest.
The devices are a block of a 4x4x8 slice.
Arguments:
- token_act: bfloat16 [16, 1536, 768], P('dp'), parts along dimension 0
- token_cond: bfloat16 [16, 1536, 384], P('dp'), parts along dimension 0
- pair_bias: bfloat16 [2, 16, 1536, 1536], P(None, 'tp')
- token_mask: int32 [1536], replicated
- ada_scale: float32 [2, 2, 384], replicated
- ada_w: bfloat16 [2, 2, 384, 2, 768], replicated
- ada_bias: float32 [2, 2, 768], replicated
- zero_w: bfloat16 [2, 384, 2, 768], replicated
- zero_b: float32 [2, 2, 768], replicated
- w_qkvg: bfloat16 [2, 768, 4, 768], P(None, None, None, 'tp')
- b_q: float32 [2, 768], P(None, 'tp')
- w_o: bfloat16 [2, 768, 768], P(None, 'tp')
- w_up: bfloat16 [2, 768, 2, 1536], P(None, None, None, 'tp')
- w_down: bfloat16 [2, 1536, 768], P(None, 'tp')
Outputs:
- output: bfloat16 [16, 1536, 768], P('dp'), parts along dimension 0
There are 2 independent parts. The reference program is written for one: setup_inputs(seed, part) draws one part's arguments, and reference() takes and returns one part's arrays. A program takes and returns all parts, laid end to end along the dimension named above; an argument that names none is the same for every part.
All inputs are finite; a program needn't handle non-finite values.
Results may differ from the reference program's by a relative error of at most 0.0179886.
Values are sent between devices in bfloat16 or wider.
A program may use at most 768 MiB of HBM per device.

```python
import math
import jax
import jax.numpy as jnp
from jax import lax

SAMPLES = 8
TOKENS = 1536
TOKEN_DIM = 768
COND_DIM = 384
NUM_HEADS = 16
HEAD_DIM = 48
HIDDEN_DIM = 1536
BLOCKS = 2

LN_EPS = 1e-5
BIAS_SCALE = math.sqrt(math.log(TOKENS / 4.0))


def layer_norm(values_in):
    row_mean = jnp.mean(values_in, axis=-1, keepdims=True)
    centered = values_in - row_mean
    variance = jnp.mean(centered * centered, axis=-1, keepdims=True)
    return centered * lax.rsqrt(variance + LN_EPS)


def ada_norm(act_f32, cond_normed, scale_vec, weight, bias_vec):
    cond_in = (cond_normed * scale_vec).astype(jnp.bfloat16)
    modulation = jnp.dot(cond_in, weight.reshape(COND_DIM, 2 * TOKEN_DIM), preferred_element_type=jnp.float32)
    modulation = modulation.reshape(-1, 2, TOKEN_DIM)
    return (jax.nn.sigmoid(modulation[:, 0] + bias_vec) * layer_norm(act_f32) + modulation[:, 1]).astype(jnp.bfloat16)


def setup_inputs(seed: int = 0, part: int = 0) -> dict:
    root_key = jax.random.key(seed)
    shared_keys = jax.random.split(root_key, 12)
    part_keys = jax.random.split(jax.random.fold_in(shared_keys[11], part), 2)
    token_act = jax.random.normal(part_keys[0], (SAMPLES, TOKENS, TOKEN_DIM), jnp.float32)
    token_cond = jax.random.normal(part_keys[1], (SAMPLES, TOKENS, COND_DIM), jnp.float32)
    pair_bias = BIAS_SCALE * jax.random.normal(shared_keys[0], (BLOCKS, NUM_HEADS, TOKENS, TOKENS), jnp.float32)
    keep_draw = jax.random.randint(shared_keys[1], (TOKENS,), 0, 4)
    token_mask = jnp.where((keep_draw != 0) | (jnp.arange(TOKENS) == 0), 1, 0).astype(jnp.int32)
    cond_gain = COND_DIM ** -0.5
    width_gain = TOKEN_DIM ** -0.5
    hidden_gain = HIDDEN_DIM ** -0.5
    ada_scale = 1.0 + 0.5 * jax.random.normal(shared_keys[2], (BLOCKS, 2, COND_DIM), jnp.float32)
    ada_w = cond_gain * jax.random.normal(shared_keys[3], (BLOCKS, 2, COND_DIM, 2, TOKEN_DIM), jnp.float32)
    ada_bias = jax.random.normal(shared_keys[4], (BLOCKS, 2, TOKEN_DIM), jnp.float32)
    zero_w = cond_gain * jax.random.normal(shared_keys[5], (BLOCKS, COND_DIM, 2, TOKEN_DIM), jnp.float32)
    zero_b = jax.random.normal(shared_keys[6], (BLOCKS, 2, TOKEN_DIM), jnp.float32)
    w_qkvg = width_gain * jax.random.normal(shared_keys[7], (BLOCKS, TOKEN_DIM, 4, TOKEN_DIM), jnp.float32)
    b_q = jax.random.normal(shared_keys[8], (BLOCKS, TOKEN_DIM), jnp.float32)
    w_o = 2.0 * width_gain * jax.random.normal(shared_keys[9], (BLOCKS, TOKEN_DIM, TOKEN_DIM), jnp.float32)
    up_down = jax.random.split(shared_keys[10], 2)
    w_up = width_gain * jax.random.normal(up_down[0], (BLOCKS, TOKEN_DIM, 2, HIDDEN_DIM), jnp.float32)
    w_down = 2.0 * hidden_gain * jax.random.normal(up_down[1], (BLOCKS, HIDDEN_DIM, TOKEN_DIM), jnp.float32)
    return {
        'token_act': token_act.astype(jnp.bfloat16),
        'token_cond': token_cond.astype(jnp.bfloat16),
        'pair_bias': pair_bias.astype(jnp.bfloat16),
        'token_mask': token_mask,
        'ada_scale': ada_scale,
        'ada_w': ada_w.astype(jnp.bfloat16),
        'ada_bias': ada_bias,
        'zero_w': zero_w.astype(jnp.bfloat16),
        'zero_b': zero_b,
        'w_qkvg': w_qkvg.astype(jnp.bfloat16),
        'b_q': b_q,
        'w_o': w_o.astype(jnp.bfloat16),
        'w_up': w_up.astype(jnp.bfloat16),
        'w_down': w_down.astype(jnp.bfloat16),
    }


def reference(token_act, token_cond, pair_bias, token_mask, ada_scale, ada_w, ada_bias, zero_w, zero_b, w_qkvg, b_q, w_o, w_up, w_down):
    row_count = SAMPLES * TOKENS
    head_shape = (SAMPLES, TOKENS, NUM_HEADS, HEAD_DIM)
    logit_scale = 1.0 / math.sqrt(HEAD_DIM)
    mask_add = (token_mask.astype(jnp.float32) - 1.0) * 1e9
    cond_flat = token_cond.reshape(row_count, COND_DIM)
    cond_normed = layer_norm(cond_flat.astype(jnp.float32))

    def block_step(act_flat, layer_args):
        (layer_scale, layer_ada_w, layer_ada_b, layer_zero_w, layer_zero_b, layer_qkvg, layer_bq, layer_wo, layer_up, layer_down, layer_bias) = layer_args
        out_gates = jax.nn.sigmoid(jnp.dot(cond_flat, layer_zero_w.reshape(COND_DIM, 2 * TOKEN_DIM), preferred_element_type=jnp.float32).reshape(row_count, 2, TOKEN_DIM) + layer_zero_b)
        act_f32 = act_flat.astype(jnp.float32)
        normed = ada_norm(act_f32, cond_normed, layer_scale[0], layer_ada_w[0], layer_ada_b[0])
        projected = jnp.dot(normed, layer_qkvg.reshape(TOKEN_DIM, 4 * TOKEN_DIM), preferred_element_type=jnp.float32).reshape(row_count, 4, TOKEN_DIM)
        query_rows = (projected[:, 0] + layer_bq).astype(jnp.bfloat16).reshape(head_shape)
        key_rows = projected[:, 1].astype(jnp.bfloat16).reshape(head_shape)
        value_rows = projected[:, 2].astype(jnp.bfloat16).reshape(head_shape)
        gate_heads = jax.nn.sigmoid(projected[:, 3])
        bias_f32 = layer_bias.astype(jnp.float32)

        def attend(operands):
            query_one, key_one, value_one = operands
            logits = jnp.einsum('qhc,khc->hqk', query_one.astype(jnp.float32), key_one.astype(jnp.float32)) * logit_scale + bias_f32 + mask_add
            attn_probs = jax.nn.softmax(logits, axis=-1).astype(jnp.bfloat16)
            return jnp.einsum('hqk,khc->qhc', attn_probs.astype(jnp.float32), value_one.astype(jnp.float32))

        mixed_heads = lax.map(attend, (query_rows, key_rows, value_rows)).reshape(row_count, TOKEN_DIM)
        heads_out = (gate_heads * mixed_heads).astype(jnp.bfloat16)
        attn_out = jnp.dot(heads_out, layer_wo, preferred_element_type=jnp.float32).astype(jnp.bfloat16).astype(jnp.float32)
        mid_f32 = (act_f32 + out_gates[:, 0] * attn_out).astype(jnp.bfloat16).astype(jnp.float32)
        normed_mid = ada_norm(mid_f32, cond_normed, layer_scale[1], layer_ada_w[1], layer_ada_b[1])
        hidden_pre = jnp.dot(normed_mid, layer_up.reshape(TOKEN_DIM, 2 * HIDDEN_DIM), preferred_element_type=jnp.float32).reshape(row_count, 2, HIDDEN_DIM)
        hidden = (jax.nn.silu(hidden_pre[:, 0]) * hidden_pre[:, 1]).astype(jnp.bfloat16)
        trans_out = jnp.dot(hidden, layer_down, preferred_element_type=jnp.float32).astype(jnp.bfloat16).astype(jnp.float32)
        act_next = (mid_f32 + out_gates[:, 1] * trans_out).astype(jnp.bfloat16)
        return act_next, None

    layer_stack = (ada_scale, ada_w, ada_bias, zero_w, zero_b, w_qkvg, b_q, w_o, w_up, w_down, pair_bias)
    final_act = lax.scan(block_step, token_act.reshape(row_count, TOKEN_DIM), layer_stack)[0]
    return final_act.reshape(SAMPLES, TOKENS, TOKEN_DIM)
```

```python
import functools
import math

import jax
import jax.numpy as jnp
import numpy as np
from jax import lax
from jax.experimental import pallas as pl
from jax.experimental.pallas import tpu as pltpu
from jax.sharding import PartitionSpec as P

LN_EPS = 1e-5
LOG2E = math.log2(math.e)
MASK_VALUE = 1e9
BLOCK = 128
QUERY_TILE = 256
KEY_TILE = 256
SCORE_TILE = 768
ROW_TILE = 512
HIDDEN_TILE = 512
CHUNK_SAMPLES = 2
LANES = 128
SUBLANES = 8
F32 = jnp.float32
BF16 = jnp.bfloat16


def dot(a, b):
    return jnp.dot(a, b, preferred_element_type=F32)


def dot_nt(a, b):
    return lax.dot_general(a, b, (((1,), (1,)), ((), ())), preferred_element_type=F32)


def dot_tn(a, b):
    return lax.dot_general(a, b, (((0,), (0,)), ((), ())), preferred_element_type=F32)


def sigmoid(x):
    return 0.5 * jnp.tanh(0.5 * x) + 0.5


def layer_norm(x):
    centered = x - jnp.mean(x, axis=-1, keepdims=True)
    variance = jnp.mean(centered * centered, axis=-1, keepdims=True)
    return centered * lax.rsqrt(variance + LN_EPS)


def mask_terms():
    left = np.float32(-MASK_VALUE * LOG2E)
    terms = []
    for _ in range(3):
        term = np.float32(np.asarray(left).astype(BF16))
        terms.append(float(term))
        left = np.float32(left - term)
    return terms


def cost(flops, bytes_accessed):
    return pl.CostEstimate(flops=int(flops), bytes_accessed=int(bytes_accessed), transcendentals=0)


def ada_norm(x_normed, cond_normed, scale, weight, bias):
    cond_in = (cond_normed * scale).astype(BF16)
    width = x_normed.shape[-1]
    parts = []
    for at in range(0, width, 256):
        gate = dot(cond_in, weight(0, at, 256))
        shift = dot(cond_in, weight(1, at, 256))
        parts.append((sigmoid(gate + bias[:, at:at + 256]) * x_normed[:, at:at + 256] + shift).astype(BF16))
    return jnp.concatenate(parts, axis=-1)


def write_projection(x1, w_ref, b_q_ref, mask_ref, q_ref, k_ref, v_ref, g_ref, head_dim, heads):
    used = heads * head_dim
    rows = x1.shape[0]
    made = dot_nt(w_ref[...], x1)
    query = (made[:used] + b_q_ref[...]).astype(BF16).astype(F32) * (LOG2E / math.sqrt(head_dim))
    high = query.astype(BF16)
    low = (query - high.astype(F32)).astype(BF16)
    row = lax.broadcasted_iota(jnp.int32, (LANES - used, rows), 0)
    ones = jnp.where(row < 3, 1.0, 0.0).astype(BF16)
    q_ref[0, :used] = high
    q_ref[0, used:LANES] = ones
    q_ref[0, LANES:LANES + used] = low
    q_ref[0, LANES + used:] = jnp.zeros_like(ones)
    keys = jnp.concatenate([made[used:2 * used], jnp.zeros((LANES - used, rows), F32)], axis=0).T
    k_ref[...] = (keys.astype(BF16).astype(F32) + mask_ref[...].astype(F32)).astype(BF16)
    v_ref[...] = made[2 * used:3 * used].astype(BF16).reshape(v_ref.shape)
    g_ref[...] = sigmoid(made[3 * used:]).reshape(g_ref.shape)


def first_kernel(act_ref, cond_ref, scale_ref, ada_w_ref, bias_ref, w_ref, b_q_ref, mask_ref, q_ref, k_ref, v_ref, g_ref, *, head_dim, heads):
    cond_normed = layer_norm(cond_ref[...].astype(F32))
    x_normed = layer_norm(act_ref[...].astype(F32))
    x1 = ada_norm(x_normed, cond_normed, scale_ref[...], lambda g, at, n: ada_w_ref[g, :, at:at + n], bias_ref[...])
    write_projection(x1, w_ref, b_q_ref, mask_ref, q_ref, k_ref, v_ref, g_ref, head_dim, heads)


def next_kernel(x1_ref, w_ref, b_q_ref, mask_ref, q_ref, k_ref, v_ref, g_ref, *, head_dim, heads):
    x1 = x1_ref[...].reshape(k_ref.shape[0], x1_ref.shape[-1])
    write_projection(x1, w_ref, b_q_ref, mask_ref, q_ref, k_ref, v_ref, g_ref, head_dim, heads)


def attend_kernel(bias_ref, q_ref, k_ref, v_ref, g_ref, out_ref, bias_t, scores_a, scores_b, send, send_sem, recv_sem, *, devices, head_dim, heads):
    tile, head = pl.program_id(0), pl.program_id(1)
    tiles = pl.num_programs(0)
    samples, tokens = k_ref.shape[0], k_ref.shape[1]
    blocks = tokens // BLOCK
    per_tile = QUERY_TILE // BLOCK
    slots = out_ref.shape[1]
    key_tiles = tokens // KEY_TILE
    me = lax.axis_index('tp')
    parity = lax.rem(tile, 2)
    row = lax.rem(lax.broadcasted_iota(jnp.int32, (2 * LANES, QUERY_TILE), 0), LANES)
    mine = ((row >= head * head_dim) & (row < (head + 1) * head_dim)) | (row >= heads * head_dim)

    def peer(step):
        return lax.rem(me + step, devices)

    def where_to(at_tile, sample, i):
        block = sample * blocks + at_tile * per_tile + i
        return lax.rem(block, devices), lax.div(block, devices)

    def local(at_tile, sample, i, slot):
        p = lax.rem(at_tile, 2)
        return pltpu.make_async_copy(send.at[p, sample, i], out_ref.at[me, slot], send_sem.at[p, sample, i])

    def remote(at_tile, sample, i, to, slot):
        p = lax.rem(at_tile, 2)
        return pltpu.make_async_remote_copy(
            src_ref=send.at[p, sample, i], dst_ref=out_ref.at[me, slot], send_sem=send_sem.at[p, sample, i],
            recv_sem=recv_sem.at[slot, me], device_id={'tp': to}, device_id_type=pl.DeviceIdType.MESH)

    def each(at_tile, local_do, remote_do):
        @pl.loop(0, samples)
        def _(sample):
            for i in range(per_tile):
                to, slot = where_to(at_tile, sample, i)

                @pl.when(to == me)
                def _():
                    local_do(local(at_tile, sample, i, slot))

                @pl.when(to != me)
                def _():
                    remote_do(remote(at_tile, sample, i, to, slot))

    @pl.when((tile == 0) & (head == 0))
    def _():
        barrier = pltpu.get_barrier_semaphore()
        for step in range(1, devices):
            pl.semaphore_signal(barrier, inc=1, device_id={'tp': peer(step)}, device_id_type=pl.DeviceIdType.MESH)
        pl.semaphore_wait(barrier, devices - 1)

    @pl.when((tile >= 2) & (head == 0))
    def _():
        each(tile - 2, lambda c: c.wait(), lambda c: c.wait_send())

    for at in range(0, tokens, KEY_TILE):
        bias_t[at:at + KEY_TILE, :] = bias_ref[:, at:at + KEY_TILE].astype(F32).T * LOG2E

    def score(sample, scores, kt, queries, top):
        at = kt * SCORE_TILE
        keys = k_ref[sample, at:at + SCORE_TILE, :]
        logits = dot(jnp.concatenate([keys, keys], axis=1), queries) + bias_t[at:at + SCORE_TILE, :]
        scores[at:at + SCORE_TILE, :] = logits
        part = jnp.max(logits.reshape(SCORE_TILE // SUBLANES, SUBLANES, QUERY_TILE), axis=0)
        return part if top is None else jnp.maximum(top, part)

    def queries_of(sample):
        return jnp.where(mine, q_ref[sample].astype(F32), 0.0).astype(BF16)

    def mix(sample, scores, kt, top, total, mixed):
        at = kt * KEY_TILE
        weights = jnp.exp2(scores[at:at + KEY_TILE, :] - top)
        part = jnp.sum(weights.reshape(KEY_TILE // SUBLANES, SUBLANES, QUERY_TILE), axis=0)
        value = dot(v_ref[sample, head, :, at:at + KEY_TILE], weights.astype(BF16))
        return (part, value) if total is None else (total + part, mixed + value)

    def finish(sample, total, mixed):
        norm = 1.0 / jnp.sum(total, axis=0, keepdims=True)
        done = (mixed * norm * g_ref[sample, head]).astype(BF16)
        for i in range(per_tile):
            send[parity, sample, i, head] = done[:, i * BLOCK:(i + 1) * BLOCK]

    def both(ahead, scores_ahead, sample, scores, top):
        queries = queries_of(ahead) if ahead is not None else None
        top = jnp.max(top, axis=0, keepdims=True) if sample is not None else None
        next_top = total = mixed = None
        for kt in range(key_tiles):
            if ahead is not None and kt % (SCORE_TILE // KEY_TILE) == 0:
                next_top = score(ahead, scores_ahead, kt // (SCORE_TILE // KEY_TILE), queries, next_top)
            if sample is not None:
                total, mixed = mix(sample, scores, kt, top, total, mixed)
        if sample is not None:
            finish(sample, total, mixed)
        return next_top

    top = both(0, scores_a, None, None, None)

    def pair(i, top):
        top = both(2 * i + 1, scores_b, 2 * i, scores_a, top)
        return both(2 * i + 2, scores_a, 2 * i + 1, scores_b, top)

    top = lax.fori_loop(0, samples // 2 - 1, pair, top)
    top = both(samples - 1, scores_b, samples - 2, scores_a, top)
    both(None, None, samples - 1, scores_b, top)

    @pl.when(head == heads - 1)
    def _():
        each(tile, lambda c: c.start(), lambda c: c.start())

    @pl.when((tile == tiles - 1) & (head == heads - 1))
    def _():
        each(tile - 1, lambda c: c.wait(), lambda c: c.wait_send())
        each(tile, lambda c: c.wait(), lambda c: c.wait_send())
        for step in range(1, devices):
            @pl.loop(0, slots)
            def _(slot):
                pltpu.make_async_remote_copy(
                    src_ref=send.at[0, 0, 0], dst_ref=out_ref.at[peer(step), slot], send_sem=send_sem.at[0, 0, 0],
                    recv_sem=recv_sem.at[slot, peer(step)], device_id={'tp': peer(step)},
                    device_id_type=pl.DeviceIdType.MESH).wait_recv()


def rows_kernel(me_ref, mixed_ref, act_ref, cond_ref, w_ref, zero_w_ref, ada_w_ref, next_w_ref, zero_b_ref, scale_ref, bias_ref, next_scale_ref, next_bias_ref, *rest, first_row, units, local_width):
    *outs, w_up1, w_up2, w_down, w_o, w_zero, w_ada, w_next, sem = rest
    devices = w_ref.shape[0]
    width = act_ref.shape[-1]
    last = len(outs) == 1

    def part(at, n):
        return w_ref.at[:, pl.ds(first_row + at, n)]

    copies = [
        pltpu.make_async_copy(zero_w_ref, w_zero, sem.at[0]),
        pltpu.make_async_copy(part(3 * units, local_width), w_o, sem.at[1]),
        pltpu.make_async_copy(ada_w_ref, w_ada, sem.at[2]),
        pltpu.make_async_copy(part(0, units), w_up1, sem.at[3]),
        pltpu.make_async_copy(part(units, units), w_up2, sem.at[4]),
        pltpu.make_async_copy(part(2 * units, units), w_down, sem.at[5]),
    ]
    if not last:
        copies.append(pltpu.make_async_copy(next_w_ref, w_next, sem.at[6]))
    for copy in copies:
        copy.start()
    slots = act_ref.shape[0]
    rows = slots * BLOCK
    cond = cond_ref[...].reshape(rows, cond_ref.shape[-1])
    cond_normed = layer_norm(cond.astype(F32))
    copies[0].wait()
    gates = [sigmoid(dot(cond, w_zero[g]) + zero_b_ref[g:g + 1]) for g in range(2)]
    copies[1].wait()
    weights_o = w_o[...].reshape(devices * local_width, width)
    attn = jnp.concatenate([dot_tn(mixed_ref[:, s].reshape(devices * local_width, BLOCK), weights_o) for s in range(slots)], axis=0)
    mid = (act_ref[...].reshape(rows, width).astype(F32) + gates[0] * attn.astype(BF16).astype(F32)).astype(BF16).astype(F32)
    copies[2].wait()
    normed = ada_norm(layer_norm(mid), cond_normed, scale_ref[...], lambda g, at, n: w_ada[g, :, at:at + n], bias_ref[...])
    copies[3].wait()
    copies[4].wait()
    up1 = w_up1[...].reshape(devices * units, width)
    up2 = w_up2[...].reshape(devices * units, width)
    hidden = []
    for at in range(0, devices * units, HIDDEN_TILE):
        u1 = dot_nt(normed, up1[at:at + HIDDEN_TILE])
        u2 = dot_nt(normed, up2[at:at + HIDDEN_TILE])
        hidden.append((u1 * sigmoid(u1) * u2).astype(BF16))
    copies[5].wait()
    moved = dot(jnp.concatenate(hidden, axis=-1), w_down[...].reshape(devices * units, width))
    act_new = (mid + gates[1] * moved.astype(BF16).astype(F32)).astype(BF16)
    outs[0][...] = act_new.reshape(outs[0].shape)
    if not last:
        copies[6].wait()
        x1 = ada_norm(layer_norm(act_new.astype(F32)), cond_normed, next_scale_ref[...], lambda g, at, n: w_next[g, :, at:at + n], next_bias_ref[...])
        outs[1][...] = x1.reshape(outs[1].shape)


def place_kernel(part_ref, *refs):
    refs[-1][0] = part_ref[:, 0]


def solution(mesh):
    devices = mesh.shape['tp']
    any_spec = pl.BlockSpec(memory_space=pl.ANY)

    def params(*semantics, limit=None, **more):
        return pltpu.CompilerParams(dimension_semantics=semantics or None, vmem_limit_bytes=limit, **more)

    def whole(shape):
        return pl.BlockSpec(shape, lambda *_: (0,) * len(shape), pipeline_mode=pl.Buffered(1))

    def shard_body(token_act, token_cond, pair_bias, token_mask, ada_scale, ada_w, ada_bias, zero_w, zero_b, w_qkvg, b_q, w_o, w_up, w_down):
        samples, tokens, width = token_act.shape
        cond_dim = token_cond.shape[-1]
        layers, heads = pair_bias.shape[:2]
        local_width = w_qkvg.shape[-1]
        head_dim = local_width // heads
        units = w_down.shape[1]
        chunk = CHUNK_SAMPLES
        chunks = samples // chunk
        slots = chunk * tokens // (devices * BLOCK)
        all_slots = slots * chunks
        me = lax.axis_index('tp').reshape(1).astype(jnp.int32)

        local_w = jnp.concatenate([part for l in range(layers) for part in (w_up[l, :, 0].T, w_up[l, :, 1].T, w_down[l], w_o[l])], axis=0)
        full_w = lax.all_gather(local_w, 'tp')
        ada_t = [[ada_w[l, j].transpose(1, 0, 2) for j in range(2)] for l in range(layers)]
        zero_t = [zero_w[l].transpose(1, 0, 2) for l in range(layers)]
        w_proj = [w_qkvg[l].reshape(width, 4 * local_width).T for l in range(layers)]
        b_q_col = [b_q[l].reshape(local_width, 1) for l in range(layers)]
        terms = jnp.zeros((LANES,), F32)
        for i, value in enumerate(mask_terms()):
            terms = terms.at[local_width + i].set(value)
        mask_rows = jnp.where(token_mask[:, None] == 0, terms[None, :], 0.0).astype(BF16)

        tiles = tokens // ROW_TILE
        proj_specs = [whole((4 * local_width, width)), whole((local_width, 1)),
                      pl.BlockSpec((ROW_TILE, LANES), lambda i: (lax.rem(i, tiles), 0))]

        def proj_outs(n):
            rows = pl.BlockSpec((ROW_TILE, LANES), lambda i: (i, 0))
            cols = pl.BlockSpec((1, heads, head_dim, ROW_TILE), lambda i: (lax.div(i, tiles), 0, 0, lax.rem(i, tiles)))
            shape_rows = jax.ShapeDtypeStruct((n * tokens, LANES), BF16)
            query = pl.BlockSpec((1, 2 * LANES, ROW_TILE), lambda i: (lax.div(i, tiles), 0, lax.rem(i, tiles)))
            return [query, rows, cols, cols], [jax.ShapeDtypeStruct((n, 2 * LANES, tokens), BF16), shape_rows,
                                               jax.ShapeDtypeStruct((n, heads, head_dim, tokens), BF16),
                                               jax.ShapeDtypeStruct((n, heads, head_dim, tokens), F32)]

        def proj_args(l):
            return w_proj[l], b_q_col[l], mask_rows

        def first():
            specs, shapes = proj_outs(samples)
            rows = samples * tokens
            return pl.pallas_call(
                functools.partial(first_kernel, head_dim=head_dim, heads=heads),
                grid=(rows // ROW_TILE,),
                in_specs=[pl.BlockSpec((ROW_TILE, width), lambda i: (i, 0)), pl.BlockSpec((ROW_TILE, cond_dim), lambda i: (i, 0)),
                          whole((1, cond_dim)), whole((2, cond_dim, width)), whole((1, width))] + proj_specs,
                out_specs=specs, out_shape=shapes, compiler_params=params('arbitrary'), name='first',
                cost_estimate=cost(2 * rows * (cond_dim * 2 * width + width * 4 * local_width), rows * width * 6),
            )(token_act.reshape(rows, width), token_cond.reshape(rows, cond_dim), ada_scale[0, 0:1], ada_t[0][0], ada_bias[0, 0:1], *proj_args(0))

        def following(x1, l):
            specs, shapes = proj_outs(chunk)
            rows = chunk * tokens
            per = ROW_TILE // BLOCK
            turns = devices // per
            return pl.pallas_call(
                functools.partial(next_kernel, head_dim=head_dim, heads=heads),
                grid=(rows // ROW_TILE,),
                in_specs=[pl.BlockSpec((per, 1, BLOCK, width), lambda i: (lax.rem(i, turns), lax.div(i, turns), 0, 0))] + proj_specs,
                out_specs=specs, out_shape=shapes, compiler_params=params('arbitrary'), name='following',
                cost_estimate=cost(2 * rows * width * 4 * local_width, rows * width * 6),
            )(x1, *proj_args(l))

        def attend(parts, n, l, collective_id):
            q, k, v, g = parts
            query = pl.BlockSpec((n, 2 * LANES, QUERY_TILE), lambda t, h: (0, 0, t))
            n_slots = n * tokens // (devices * BLOCK)
            shaped = (n, tokens, LANES)
            per_tile = QUERY_TILE // BLOCK
            return pl.pallas_call(
                functools.partial(attend_kernel, devices=devices, head_dim=head_dim, heads=heads),
                grid=(tokens // QUERY_TILE, heads),
                in_specs=[pl.BlockSpec((None, None, QUERY_TILE, tokens), lambda t, h: (l, h, t, 0)), query,
                          whole(shaped), whole((n, heads, head_dim, tokens)),
                          pl.BlockSpec((n, heads, head_dim, QUERY_TILE), lambda t, h: (0, 0, 0, t))],
                out_specs=any_spec,
                out_shape=jax.ShapeDtypeStruct((devices, n_slots, heads, head_dim, BLOCK), BF16),
                scratch_shapes=[pltpu.VMEM((tokens, QUERY_TILE), F32), pltpu.VMEM((tokens, QUERY_TILE), F32), pltpu.VMEM((tokens, QUERY_TILE), F32),
                                pltpu.VMEM((2, n, per_tile, heads, head_dim, BLOCK), BF16),
                                pltpu.SemaphoreType.DMA((2, n, per_tile)), pltpu.SemaphoreType.DMA((n_slots, devices))],
                compiler_params=params('arbitrary', 'arbitrary', collective_id=collective_id, has_side_effects=True), name='attend',
                cost_estimate=cost(4 * n * heads * tokens * tokens * 2 * LANES, heads * tokens * tokens * 2),
            )(pair_bias, q, k.reshape(shaped), v, g)

        def rows(mixed, act, l, c):
            last = l == layers - 1
            n_rows = slots * BLOCK
            nxt = 0 if last else l + 1
            own = pl.BlockSpec((slots, None, BLOCK, width), lambda i, me: (c, me[0], 0, 0))
            if l == 0:
                act, act_spec, mixed_at = token_act.reshape(all_slots, devices, BLOCK, width), own, c
            else:
                act_spec, mixed_at = pl.BlockSpec((slots, BLOCK, width), lambda i, me: (0, 0, 0)), 0
            small = lambda n: whole((1, n))
            out_spec = pl.BlockSpec((slots, BLOCK, width), lambda i, me: (0, 0, 0))
            out_shape = jax.ShapeDtypeStruct((slots, BLOCK, width), BF16)
            n_out = 1 if last else 2
            matrix = pltpu.VMEM((2, cond_dim, width), BF16)
            ups = pltpu.VMEM((devices, units, width), BF16)
            return pl.pallas_call(
                functools.partial(rows_kernel, first_row=l * (3 * units + local_width), units=units, local_width=local_width),
                grid_spec=pltpu.PrefetchScalarGridSpec(
                    num_scalar_prefetch=1, grid=(1,),
                    in_specs=[pl.BlockSpec((devices, slots, heads, head_dim, BLOCK), lambda i, me: (0, mixed_at, 0, 0, 0)), act_spec,
                              pl.BlockSpec((slots, None, BLOCK, cond_dim), lambda i, me: (c, me[0], 0, 0)),
                              any_spec, any_spec, any_spec, any_spec,
                              whole((2, width)), small(cond_dim), small(width), small(cond_dim), small(width)],
                    out_specs=[out_spec] * n_out,
                    scratch_shapes=[ups, ups, ups, pltpu.VMEM((devices, local_width, width), BF16), matrix, matrix, matrix, pltpu.SemaphoreType.DMA((7,))]),
                out_shape=[out_shape] * n_out, compiler_params=params('arbitrary'), name='rows',
                cost_estimate=cost(2 * n_rows * width * (width + 3 * devices * units + 6 * cond_dim), devices * (3 * units + local_width) * width * 2),
            )(me, mixed, act, token_cond.reshape(all_slots, devices, BLOCK, cond_dim), full_w, zero_t[l], ada_t[l][1], ada_t[nxt][0],
              zero_b[l], ada_scale[l, 1:2], ada_bias[l, 1:2], ada_scale[nxt, 0:1], ada_bias[nxt, 0:1])

        def place(out, part, c):
            first_one = out is None
            return pl.pallas_call(
                place_kernel, grid=(slots,),
                in_specs=[pl.BlockSpec((devices, 1, BLOCK, width), lambda i: (0, i, 0, 0))] + ([] if first_one else [any_spec]),
                out_specs=pl.BlockSpec((1, devices, BLOCK, width), lambda i: (c * slots + i, 0, 0, 0)),
                out_shape=jax.ShapeDtypeStruct((all_slots, devices, BLOCK, width), BF16),
                input_output_aliases={} if first_one else {1: 0},
                compiler_params=params('arbitrary'), name='place',
            )(*((part,) if first_one else (part, out)))

        mixed = attend(first(), samples, 0, 0)
        acts, x1s = [None] * chunks, [None] * chunks
        for c in range(chunks):
            acts[c], x1 = rows(mixed, None, 0, c)
            x1s[c] = lax.all_gather(x1, 'tp')
        out = None
        parts = []
        for l in range(1, layers):
            last = l == layers - 1
            for c in range(chunks):
                mixed = attend(following(x1s[c], l), chunk, l, 1 + (l - 1) * chunks + c)
                if last:
                    parts.append(lax.all_gather(rows(mixed, acts[c], l, c)[0], 'tp'))
                else:
                    acts[c], x1 = rows(mixed, acts[c], l, c)
                    x1s[c] = lax.all_gather(x1, 'tp')
        for c in range(chunks):
            out = place(out, parts[c], c)
        return out.reshape(samples, tokens, width)

    everywhere = P()
    in_specs = (P('dp', None, None), P('dp', None, None), P(None, 'tp', None, None), P(None), everywhere, everywhere, everywhere, everywhere, everywhere, P(None, None, None, 'tp'), P(None, 'tp'), P(None, 'tp', None), P(None, None, None, 'tp'), P(None, 'tp', None))
    return jax.shard_map(shard_body, mesh=mesh, in_specs=in_specs, out_specs=P('dp', None, None), check_vma=False)
```

```python
import functools
import math

import jax
import jax.numpy as jnp
import numpy as np
from jax import lax
from jax.experimental import pallas as pl
from jax.experimental.pallas import tpu as pltpu
from jax.sharding import PartitionSpec as P

LN_EPS = 1e-5
LOG2E = math.log2(math.e)
MASK_VALUE = 1e9
BLOCK = 128
QUERY_TILE = 256
KEY_TILE = 256
SCORE_TILE = 256
ROW_TILE = 512
HIDDEN_TILE = 512
CHUNK_SAMPLES = 2
LANES = 128
SUBLANES = 8
F32 = jnp.float32
BF16 = jnp.bfloat16


def dot(a, b):
    return jnp.dot(a, b, preferred_element_type=F32)


def dot_nt(a, b):
    return lax.dot_general(a, b, (((1,), (1,)), ((), ())), preferred_element_type=F32)


def dot_tn(a, b):
    return lax.dot_general(a, b, (((0,), (0,)), ((), ())), preferred_element_type=F32)


def sigmoid(x):
    return 0.5 * jnp.tanh(0.5 * x) + 0.5


def layer_norm(x):
    centered = x - jnp.mean(x, axis=-1, keepdims=True)
    variance = jnp.mean(centered * centered, axis=-1, keepdims=True)
    return centered * lax.rsqrt(variance + LN_EPS)


def mask_terms():
    left = np.float32(-MASK_VALUE * LOG2E)
    terms = []
    for _ in range(3):
        term = np.float32(np.asarray(left).astype(BF16))
        terms.append(float(term))
        left = np.float32(left - term)
    return terms


def cost(flops, bytes_accessed):
    return pl.CostEstimate(flops=int(flops), bytes_accessed=int(bytes_accessed), transcendentals=0)


def ada_norm(x_normed, cond_normed, scale, weight, bias):
    cond_in = (cond_normed * scale).astype(BF16)
    width = x_normed.shape[-1]
    parts = []
    for at in range(0, width, 256):
        gate = dot(cond_in, weight(0, at, 256))
        shift = dot(cond_in, weight(1, at, 256))
        parts.append((sigmoid(gate + bias[:, at:at + 256]) * x_normed[:, at:at + 256] + shift).astype(BF16))
    return jnp.concatenate(parts, axis=-1)


def bounds(at, size, step=LANES):
    return pl.ds(pl.multiple_of(at, step), size)


def write_projection(x1, w_ref, b_q, mask, q_ref, k_ref, v_ref, g_ref, sample, at, head_dim, heads):
    used = heads * head_dim
    rows = x1.shape[0]
    spare = LANES - used
    here = bounds(at, rows)
    made = dot_nt(w_ref[...], x1)
    query = (made[:used] + b_q).astype(BF16).astype(F32) * (LOG2E / math.sqrt(head_dim))
    high = query.astype(BF16)
    low = (query - high.astype(F32)).astype(BF16)
    row = lax.broadcasted_iota(jnp.int32, (spare, rows), 0)
    ones = jnp.where(row < 3, 1.0, 0.0).astype(BF16)
    q_ref[sample, :used, here] = high
    q_ref[sample, used:LANES, here] = ones
    q_ref[sample, LANES:LANES + used, here] = low
    q_ref[sample, LANES + used:, here] = jnp.zeros_like(ones)
    first, second, third = mask_terms()
    masked = jnp.where(row == 0, first, jnp.where(row == 1, second, jnp.where(row == 2, third, 0.0)))
    masked = jnp.where(mask == 0, masked, 0.0)
    k_ref[sample, here, :] = jnp.concatenate([made[used:2 * used], masked], axis=0).T.astype(BF16)
    values = made[2 * used:3 * used].astype(BF16)
    gates = sigmoid(made[3 * used:])
    for h in range(heads):
        v_ref[sample, h, :, here] = values[h * head_dim:(h + 1) * head_dim]
        g_ref[sample, h, :, here] = gates[h * head_dim:(h + 1) * head_dim]


class Attention:
    def __init__(self, q_ref, k_ref, v_ref, g_ref, bias_first, bias_here, bias_next, bias_t, scores, top_ref, send, head_dim):
        self.q, self.k, self.v, self.g = q_ref, k_ref, v_ref, g_ref
        self.bias_first, self.bias_here, self.bias_next = bias_first, bias_here, bias_next
        self.bias_t, self.scores, self.top, self.send = bias_t, scores, top_ref, send
        self.head_dim = head_dim
        self.samples, self.tokens = k_ref.shape[0], k_ref.shape[1]
        self.heads = len(bias_t)
        self.tiles = self.tokens // QUERY_TILE

    def turn(self, block, h, at, size):
        for step in range(0, size, LANES):
            keys = bounds(at + step, LANES)
            self.bias_t[h][keys, :] = block[:, keys].astype(F32).T * LOG2E

    def queries(self, sample, tile, h):
        q = self.q[sample, :, bounds(tile * QUERY_TILE, QUERY_TILE)]
        used = self.heads * self.head_dim
        none = jnp.zeros((self.head_dim, QUERY_TILE), BF16)
        parts = []
        for base in (0, LANES):
            for other in range(self.heads):
                parts.append(q[base + other * self.head_dim:base + (other + 1) * self.head_dim] if other == h else none)
            parts.append(q[base + used:base + LANES])
        return jnp.concatenate(parts, axis=0)

    def score(self, unit, slot, queries, kt, top):
        sample, _, h = unit
        at = kt * SCORE_TILE
        keys = self.k[sample, at:at + SCORE_TILE, :]
        logits = dot(jnp.concatenate([keys, keys], axis=1), queries) + self.bias_t[h][at:at + SCORE_TILE, :]
        self.scores[slot][at:at + SCORE_TILE, :] = logits
        part = jnp.max(logits.reshape(SCORE_TILE // SUBLANES, SUBLANES, QUERY_TILE), axis=0)
        return part if top is None else jnp.maximum(top, part)

    def mix(self, unit, slot, top, kt, total, mixed):
        sample, _, h = unit
        at = kt * KEY_TILE
        weights = jnp.exp2(self.scores[slot][at:at + KEY_TILE, :] - top)
        part = jnp.sum(weights.reshape(KEY_TILE // SUBLANES, SUBLANES, QUERY_TILE), axis=0)
        value = dot(self.v[sample, h, :, at:at + KEY_TILE], weights.astype(BF16))
        return (part, value) if total is None else (total + part, mixed + value)

    def finish(self, unit, total, mixed):
        sample, tile, h = unit
        norm = 1.0 / jnp.sum(total, axis=0, keepdims=True)
        done = (mixed * norm * self.g[sample, h, :, bounds(tile * QUERY_TILE, QUERY_TILE)]).astype(BF16)
        for i in range(QUERY_TILE // BLOCK):
            self.send[lax.rem(tile, 2), sample, i, h] = done[:, i * BLOCK:(i + 1) * BLOCK]

    def half(self, ahead, unit, slot, top):
        queries = self.queries(*ahead)
        next_top = total = mixed = None
        if unit is not None:
            top = jnp.max(top, axis=0, keepdims=True)
        per = SCORE_TILE // KEY_TILE
        for kt in range(self.tokens // KEY_TILE):
            if kt % per == 0:
                next_top = self.score(ahead, 1 - slot, queries, kt // per, next_top)
            if unit is not None:
                total, mixed = self.mix(unit, slot, top, kt, total, mixed)
        if unit is not None:
            self.finish(unit, total, mixed)
        return next_top

    def begin(self):
        self.turn(self.bias_first, 0, 0, self.tokens)
        self.top[...] = self.half((0, 0, 0), None, 1, None)

    def step(self, tile):
        pairs = self.samples // 2
        size = self.tokens // pairs
        next_tile = lax.rem(tile + 1, self.tiles)
        top = self.top[...]
        for h in range(self.heads):
            block, other = (self.bias_here, h + 1) if h + 1 < self.heads else (self.bias_next, 0)

            def pair(i, top, ahead):
                self.turn(block, other, i * size, size)
                top = self.half((2 * i + 1, tile, h), (2 * i, tile, h), 0, top)
                return self.half(ahead, (2 * i + 1, tile, h), 1, top)

            if pairs > 1:
                top = lax.fori_loop(0, pairs - 1, lambda i, top: pair(i, top, (2 * i + 2, tile, h)), top)
            after = (0, tile, h + 1) if h + 1 < self.heads else (0, next_tile, 0)
            top = pair(pairs - 1, top, after)
        self.top[...] = top


class Exchange:
    def __init__(self, send, out_ref, send_sem, recv_sem, samples, tokens, devices):
        self.send, self.out, self.send_sem, self.recv_sem = send, out_ref, send_sem, recv_sem
        self.samples, self.blocks, self.devices = samples, tokens // BLOCK, devices
        self.me = lax.axis_index('tp')

    def copies(self, tile, local_do, remote_do):
        parity = lax.rem(tile, 2)

        @pl.loop(0, self.samples)
        def _(sample):
            for i in range(QUERY_TILE // BLOCK):
                block = sample * self.blocks + tile * (QUERY_TILE // BLOCK) + i
                to, slot = lax.rem(block, self.devices), lax.div(block, self.devices)
                source, sem = self.send.at[parity, sample, i], self.send_sem.at[parity, sample, i]

                @pl.when(to == self.me)
                def _():
                    local_do(pltpu.make_async_copy(source, self.out.at[self.me, slot], sem))

                @pl.when(to != self.me)
                def _():
                    remote_do(pltpu.make_async_remote_copy(
                        src_ref=source, dst_ref=self.out.at[self.me, slot], send_sem=sem, recv_sem=self.recv_sem.at[slot, self.me],
                        device_id={'tp': to}, device_id_type=pl.DeviceIdType.MESH))

    def start(self, tile):
        self.copies(tile, lambda c: c.start(), lambda c: c.start())

    def sent(self, tile):
        self.copies(tile, lambda c: c.wait(), lambda c: c.wait_send())

    def received(self):
        for step in range(1, self.devices):
            source = lax.rem(self.me + step, self.devices)

            @pl.loop(0, self.out.shape[1])
            def _(slot):
                pltpu.make_async_remote_copy(
                    src_ref=self.send.at[0, 0, 0], dst_ref=self.out.at[source, slot], send_sem=self.send_sem.at[0, 0, 0],
                    recv_sem=self.recv_sem.at[slot, source], device_id={'tp': source}, device_id_type=pl.DeviceIdType.MESH).wait_recv()


def signal_all(devices):
    me = lax.axis_index('tp')
    barrier = pltpu.get_barrier_semaphore()
    for step in range(1, devices):
        pl.semaphore_signal(barrier, inc=1, device_id={'tp': lax.rem(me + step, devices)}, device_id_type=pl.DeviceIdType.MESH)


def wait_all(devices):
    pl.semaphore_wait(pltpu.get_barrier_semaphore(), devices - 1)


class Gather:
    def __init__(self, own, full, send_sem, recv_sem, devices):
        self.own, self.full, self.send_sem, self.recv_sem, self.devices = own, full, send_sem, recv_sem, devices
        self.me = lax.axis_index('tp')

    def at(self, step):
        return lax.rem(self.me + step + self.devices, self.devices)

    def copy(self, k):
        me, rows = self.me, self.own.shape[1]
        partner = me + 1 - 2 * lax.rem(me, 2)
        right, left, far = self.at(2), self.at(-2), self.at(4)
        lower, upper = pl.ds(0, rows // 2), pl.ds(rows // 2, rows // 2)
        source, target, to = [
            (self.own, self.full.at[me], partner),
            (self.own, self.full.at[me], right),
            (self.own, self.full.at[me], left),
            (self.full.at[left, :, lower], self.full.at[left, :, lower], right),
            (self.full.at[right, :, upper], self.full.at[right, :, upper], left),
            (self.full.at[left], self.full.at[left], partner),
            (self.full.at[right], self.full.at[right], partner),
            (self.full.at[far], self.full.at[far], partner),
        ][k]
        return pltpu.make_async_remote_copy(
            src_ref=source, dst_ref=target, send_sem=self.send_sem.at[k], recv_sem=self.recv_sem.at[k],
            device_id={'tp': to}, device_id_type=pl.DeviceIdType.MESH)

    def local(self):
        return pltpu.make_async_copy(self.own, self.full.at[self.me], self.send_sem.at[8])

    def first(self):
        for k in (1, 2, 0):
            self.copy(k).start()
        self.local().start()

    def second(self):
        self.copy(1).wait_recv()
        self.copy(3).start()
        self.copy(2).wait_recv()
        self.copy(4).start()
        self.copy(5).start()
        self.copy(6).start()

    def third(self):
        self.copy(3).wait_recv()
        self.copy(4).wait_recv()
        self.copy(7).start()

    def last(self):
        for k in (0, 5, 6, 7):
            self.copy(k).wait_recv()
        for k in range(8):
            self.copy(k).wait_send()
        self.local().wait()


def layer_start_kernel(act_ref, cond_ref, ada_ref, scale_ref, shift_ref, w_ref, b_q_ref, mask_ref, bias_first, bias_here, bias_next, out_ref,
                       q_s, k_s, v_s, g_s, bias_a, bias_b, scores_a, scores_b, top_s, send, send_sem, recv_sem, *, devices, head_dim, heads):
    i = pl.program_id(0)
    samples, tokens = k_s.shape[0], k_s.shape[1]
    per = tokens // ROW_TILE
    ahead = samples * per
    attention = Attention(q_s, k_s, v_s, g_s, bias_first, bias_here, bias_next, (bias_a, bias_b), (scores_a, scores_b), top_s, send, head_dim)
    exchange = Exchange(send, out_ref, send_sem, recv_sem, samples, tokens, devices)
    tile = i - ahead

    @pl.when(i == 0)
    def _():
        signal_all(devices)

    @pl.when(i < ahead)
    def _():
        cond_normed = layer_norm(cond_ref[...].astype(F32))
        x_normed = layer_norm(act_ref[...].astype(F32))
        x1 = ada_norm(x_normed, cond_normed, scale_ref[0, 0:1], lambda g, at, n: ada_ref[g, :, at:at + n], shift_ref[0, 0:1])
        write_projection(x1, w_ref, b_q_ref[...], mask_ref[...], q_s, k_s, v_s, g_s, lax.div(i, per), lax.rem(i, per) * ROW_TILE, head_dim, heads)

    @pl.when(i == ahead)
    def _():
        attention.begin()
        wait_all(devices)

    @pl.when(tile >= 2)
    def _():
        exchange.sent(tile - 2)

    @pl.when(i >= ahead)
    def _():
        attention.step(tile)
        exchange.start(tile)

    @pl.when(tile == attention.tiles - 1)
    def _():
        exchange.sent(tile - 1)
        exchange.sent(tile)
        exchange.received()


class Weights:
    def __init__(self, up_ref, down_ref, o_ref, zero_ref, ada_ref, layer, next_layer, scratch, sem):
        self.up1, self.up2, self.down, self.o, self.zero, self.ada, self.next = scratch
        units, local_width = self.down.shape[1], self.o.shape[1]
        pairs = [
            (zero_ref.at[layer], self.zero), (o_ref.at[:, pl.ds(layer * local_width, local_width)], self.o), (ada_ref.at[layer, 1], self.ada),
            (up_ref.at[:, pl.ds(2 * layer * units, units)], self.up1), (up_ref.at[:, pl.ds((2 * layer + 1) * units, units)], self.up2),
            (down_ref.at[:, pl.ds(layer * units, units)], self.down)]
        if next_layer is not None:
            pairs.append((ada_ref.at[next_layer, 0], self.next))
        self.copies = [pltpu.make_async_copy(a, b, sem.at[n]) for n, (a, b) in enumerate(pairs)]

    def start(self):
        for copy in self.copies:
            copy.start()

    def wait(self, *which):
        for n in which:
            self.copies[n].wait()


def row_stage(cond, act, mixed, weights, arrived, zero_b_ref, scale_ref, shift_ref, layer, next_layer, wait):
    cond_normed = layer_norm(cond.astype(F32))
    wait(0)
    gates = [sigmoid(dot(cond, weights.zero[g]) + zero_b_ref[layer, g:g + 1]) for g in range(2)]
    wait(1)
    arrived()
    width = act.shape[-1]
    w_o = weights.o[...].reshape(-1, width)
    attn = jnp.concatenate([dot_tn(block, w_o) for block in mixed()], axis=0)
    mid = (act.astype(F32) + gates[0] * attn.astype(BF16).astype(F32)).astype(BF16).astype(F32)
    wait(2)
    normed = ada_norm(layer_norm(mid), cond_normed, scale_ref[layer, 1:2], lambda g, at, n: weights.ada[g, :, at:at + n], shift_ref[layer, 1:2])
    wait(3, 4)
    up1, up2 = weights.up1[...].reshape(-1, width), weights.up2[...].reshape(-1, width)
    hidden = []
    for at in range(0, up1.shape[0], HIDDEN_TILE):
        u1 = dot_nt(normed, up1[at:at + HIDDEN_TILE])
        u2 = dot_nt(normed, up2[at:at + HIDDEN_TILE])
        hidden.append((u1 * sigmoid(u1) * u2).astype(BF16))
    wait(5)
    moved = dot(jnp.concatenate(hidden, axis=-1), weights.down[...].reshape(-1, width))
    act_new = (mid + gates[1] * moved.astype(BF16).astype(F32)).astype(BF16)
    if next_layer is None:
        return act_new, None
    wait(6)
    return act_new, ada_norm(layer_norm(act_new.astype(F32)), cond_normed, scale_ref[next_layer, 0:1], lambda g, at, n: weights.next[g, :, at:at + n], shift_ref[next_layer, 0:1])


def rows_kernel(mixed_ref, act_ref, cond_ref, up_ref, down_ref, o_ref, zero_ref, ada_ref, zero_b_ref, scale_ref, shift_ref, act_out, x1_out, full_out,
                mixed_s, act_s, cond_s, x1_s, *rest, devices, layer, next_layer):
    *scratch, weight_sem, load_sem, send_sem, recv_sem = rest
    c = pl.program_id(0)
    slots, width = x1_s.shape[0], x1_s.shape[-1]
    rows = slots * BLOCK
    me = lax.axis_index('tp')
    weights = Weights(up_ref, down_ref, o_ref, zero_ref, ada_ref, layer, next_layer, scratch, weight_sem)
    loads = [pltpu.make_async_copy(cond_ref.at[:, me], cond_s, load_sem.at[0]),
             pltpu.make_async_copy(mixed_ref, mixed_s, load_sem.at[1]),
             pltpu.make_async_copy(act_ref.at[:, me], act_s, load_sem.at[2])]
    gather = Gather(x1_s, full_out, send_sem, recv_sem, devices)

    @pl.when(c == 0)
    def _():
        signal_all(devices)
        for load in loads[:1]:
            load.start()
        weights.copies[0].start()
        for load in loads[1:]:
            load.start()
        for copy in weights.copies[1:]:
            copy.start()
        for load in loads:
            load.wait()
        weights.wait(*range(len(weights.copies)))

    here = pl.ds(c * slots, slots)
    act_new, x1 = row_stage(
        cond_s[here].reshape(rows, cond_s.shape[-1]), act_s[here].reshape(rows, width),
        lambda: [mixed_s[:, c * slots + s].reshape(-1, BLOCK) for s in range(slots)],
        weights, lambda: None, zero_b_ref, scale_ref, shift_ref, layer, next_layer, lambda *_: None)
    act_out[...] = act_new.reshape(act_out.shape)
    x1_out[...] = x1.reshape(x1_out.shape)

    @pl.when(c == 0)
    def _():
        x1_s[...] = x1.reshape(x1_s.shape)
        wait_all(devices)
        gather.first()

    @pl.when(c == pl.num_programs(0) - 2)
    def _():
        gather.second()

    @pl.when(c == pl.num_programs(0) - 1)
    def _():
        gather.third()
        gather.last()


def layer_kernel(x1_ref, act_ref, *refs, devices, head_dim, heads, layer, chunk_at, gathers):
    if gathers:
        own_ref, *refs = refs
    cond_ref, up_ref, down_ref, o_ref, zero_ref, ada_ref, zero_b_ref, scale_ref, shift_ref, w_ref, b_q_ref, mask_ref, bias_first, bias_here, bias_next, act_out, *refs = refs
    if gathers:
        full_out, *refs = refs
    q_s, k_s, v_s, g_s, bias_a, bias_b, scores_a, scores_b, top_s, send, mixed_s, cond_s, *refs = refs
    *scratch, weight_sem, load_sem, out_sem, in_sem, send_sem, recv_sem = refs
    i = pl.program_id(0)
    samples, tokens = k_s.shape[0], k_s.shape[1]
    per = tokens // ROW_TILE
    ahead = samples * per
    slots, _, width = act_ref.shape
    rows = slots * BLOCK
    me = lax.axis_index('tp')
    attention = Attention(q_s, k_s, v_s, g_s, bias_first, bias_here, bias_next, (bias_a, bias_b), (scores_a, scores_b), top_s, send, head_dim)
    exchange = Exchange(send, mixed_s, out_sem, in_sem, samples, tokens, devices)
    weights = Weights(up_ref, down_ref, o_ref, zero_ref, ada_ref, layer, None, list(scratch) + [None], weight_sem)
    load = pltpu.make_async_copy(cond_ref.at[pl.ds(chunk_at, slots), me], cond_s, load_sem.at[0])
    gather = Gather(own_ref, full_out, send_sem, recv_sem, devices) if gathers else None
    tile = i - ahead

    @pl.when(i == 0)
    def _():
        signal_all(devices)
        load.start()
        weights.start()

    @pl.when(i < ahead)
    def _():
        x1 = x1_ref[...].reshape(ROW_TILE, width)
        write_projection(x1, w_ref, b_q_ref[...], mask_ref[...], q_s, k_s, v_s, g_s, lax.div(i, per), lax.rem(i, per) * ROW_TILE, head_dim, heads)

    @pl.when(i == 0)
    def _():
        wait_all(devices)
        if gathers:
            gather.first()

    @pl.when(i == ahead)
    def _():
        attention.begin()

    @pl.when(tile >= 2)
    def _():
        exchange.sent(tile - 2)

    @pl.when(i >= ahead)
    def _():
        attention.step(tile)
        exchange.start(tile)

    if gathers:
        @pl.when(tile == attention.tiles - 2)
        def _():
            gather.second()

    @pl.when(tile == attention.tiles - 1)
    def _():
        load.wait()

        def arrived():
            exchange.sent(tile - 1)
            exchange.sent(tile)
            exchange.received()

        act_new, _ = row_stage(
            cond_s[...].reshape(rows, cond_s.shape[-1]), act_ref[...].reshape(rows, width),
            lambda: [mixed_s[:, s].reshape(-1, BLOCK) for s in range(slots)],
            weights, arrived, zero_b_ref, scale_ref, shift_ref, layer, None, weights.wait)
        act_out[...] = act_new.reshape(act_out.shape)
        if gathers:
            gather.third()
            gather.last()


def place_kernel(part_ref, *refs):
    refs[-1][0] = part_ref[:, 0]


def solution(mesh):
    devices = mesh.shape['tp']
    any_spec = pl.BlockSpec(memory_space=pl.ANY)

    def params(**more):
        return pltpu.CompilerParams(dimension_semantics=('arbitrary',), **more)

    def whole(shape):
        return pl.BlockSpec(shape, lambda *_: (0,) * len(shape), pipeline_mode=pl.Buffered(1))

    def shard_body(token_act, token_cond, pair_bias, token_mask, ada_scale, ada_w, ada_bias, zero_w, zero_b, w_qkvg, b_q, w_o, w_up, w_down):
        samples, tokens, width = token_act.shape
        cond_dim = token_cond.shape[-1]
        layers, heads = pair_bias.shape[:2]
        local_width = w_qkvg.shape[-1]
        head_dim = local_width // heads
        units = w_down.shape[1]
        chunk = CHUNK_SAMPLES
        chunks = samples // chunk
        slots = chunk * tokens // (devices * BLOCK)
        all_slots = slots * chunks
        tiles = tokens // ROW_TILE
        q_tiles = tokens // QUERY_TILE

        full_o = lax.all_gather(w_o.reshape(layers * local_width, width), 'tp')
        full_up = lax.all_gather(w_up.transpose(0, 2, 3, 1).reshape(layers * 2 * units, width), 'tp')
        full_down = lax.all_gather(w_down.reshape(layers * units, width), 'tp')
        ada_t = ada_w.transpose(0, 1, 3, 2, 4)
        zero_t = zero_w.transpose(0, 2, 1, 3)
        w_proj = w_qkvg.transpose(0, 2, 3, 1).reshape(layers, 4 * local_width, width)
        b_q_col = b_q.reshape(layers, local_width, 1)
        mask_row = token_mask.reshape(1, tokens)
        cond_rows = token_cond.reshape(all_slots, devices, BLOCK, cond_dim)
        act_rows = token_act.reshape(all_slots, devices, BLOCK, width)

        def layer_block(l, shape):
            return pl.BlockSpec((None,) + shape, lambda *_: (l,) + (0,) * len(shape), pipeline_mode=pl.Buffered(1))

        vectors = [whole(ada_scale.shape), whole(ada_bias.shape)]

        def proj_specs(l, ahead):
            return [layer_block(l, (4 * local_width, width)), layer_block(l, (local_width, 1)),
                    pl.BlockSpec((1, ROW_TILE), lambda i: (0, lax.rem(jnp.minimum(i, ahead - 1), tiles)))]

        def bias_specs(l, ahead):
            def at(h, of):
                return pl.BlockSpec((None, None, QUERY_TILE, tokens), lambda i: (l, h, of(jnp.maximum(i - ahead, 0)), 0))
            return [pl.BlockSpec((None, None, QUERY_TILE, tokens), lambda i: (l, 0, 0, 0), pipeline_mode=pl.Buffered(1)),
                    at(heads - 1, lambda t: t), at(0, lambda t: jnp.minimum(t + 1, q_tiles - 1))]

        def attention_scratch(n):
            square = pltpu.VMEM((tokens, QUERY_TILE), F32)
            return [pltpu.VMEM((n, 2 * LANES, tokens), BF16), pltpu.VMEM((n, tokens, LANES), BF16),
                    pltpu.VMEM((n, heads, head_dim, tokens), BF16), pltpu.VMEM((n, heads, head_dim, tokens), F32),
                    square, square, square, square, pltpu.VMEM((SUBLANES, QUERY_TILE), F32),
                    pltpu.VMEM((2, n, QUERY_TILE // BLOCK, heads, head_dim, BLOCK), BF16)]

        def exchange_sems(n):
            return [pltpu.SemaphoreType.DMA((2, n, QUERY_TILE // BLOCK)), pltpu.SemaphoreType.DMA((n * tokens // (devices * BLOCK), devices))]

        matrix = pltpu.VMEM((2, cond_dim, width), BF16)
        ups = pltpu.VMEM((devices, units, width), BF16)
        row_scratch = [ups, ups, ups, pltpu.VMEM((devices, local_width, width), BF16), matrix, matrix]
        gather_sems = [pltpu.SemaphoreType.DMA((9,)), pltpu.SemaphoreType.DMA((8,))]
        row_shape = jax.ShapeDtypeStruct((slots, BLOCK, width), BF16)
        full_shape = jax.ShapeDtypeStruct((devices, slots, BLOCK, width), BF16)
        attention_flops = 4 * heads * tokens * tokens * 2 * LANES

        def layer_start():
            ahead = samples * tiles
            rows = samples * tokens
            return pl.pallas_call(
                functools.partial(layer_start_kernel, devices=devices, head_dim=head_dim, heads=heads),
                grid=(ahead + q_tiles,),
                in_specs=[pl.BlockSpec((ROW_TILE, width), lambda i: (jnp.minimum(i, ahead - 1), 0)),
                          pl.BlockSpec((ROW_TILE, cond_dim), lambda i: (jnp.minimum(i, ahead - 1), 0)),
                          pl.BlockSpec((None, None, 2, cond_dim, width), lambda i: (0, 0, 0, 0, 0), pipeline_mode=pl.Buffered(1))]
                + vectors + proj_specs(0, ahead) + bias_specs(0, ahead),
                out_specs=any_spec, out_shape=jax.ShapeDtypeStruct((devices, all_slots, heads, head_dim, BLOCK), BF16),
                scratch_shapes=attention_scratch(samples) + exchange_sems(samples),
                compiler_params=params(collective_id=0, has_side_effects=True), name='layer_start',
                cost_estimate=cost(samples * attention_flops, heads * tokens * tokens * 2 + rows * width * 4),
            )(token_act.reshape(rows, width), token_cond.reshape(rows, cond_dim), ada_t, ada_scale, ada_bias,
              w_proj, b_q_col, mask_row, pair_bias, pair_bias, pair_bias)

        def rows_of_first(mixed):
            out_spec = pl.BlockSpec((slots, BLOCK, width), lambda c: (c, 0, 0))
            out_shape = jax.ShapeDtypeStruct((all_slots, BLOCK, width), BF16)
            return pl.pallas_call(
                functools.partial(rows_kernel, devices=devices, layer=0, next_layer=1), grid=(chunks,),
                in_specs=[any_spec] * 8 + [whole(zero_b.shape)] + vectors, out_specs=[out_spec, out_spec, any_spec],
                out_shape=[out_shape, out_shape, full_shape],
                scratch_shapes=[pltpu.VMEM(mixed.shape, BF16), pltpu.VMEM((all_slots, BLOCK, width), BF16), pltpu.VMEM((all_slots, BLOCK, cond_dim), BF16),
                                pltpu.VMEM((slots, BLOCK, width), BF16)] + row_scratch + [matrix, pltpu.SemaphoreType.DMA((7,)), pltpu.SemaphoreType.DMA((3,))] + gather_sems,
                compiler_params=params(collective_id=1, has_side_effects=True), name='rows',
                cost_estimate=cost(2 * all_slots * BLOCK * width * (width + 3 * devices * units + 6 * cond_dim), devices * units * width * 6),
            )(mixed, act_rows, cond_rows, full_up, full_down, full_o, zero_t, ada_t, zero_b, ada_scale, ada_bias)

        def layer_of(x1, acts, x1s, c):
            l = 1
            ahead = chunk * tiles
            gathers = c + 1 < chunks
            per = ROW_TILE // BLOCK
            turns = devices // per

            def turn(i):
                i = jnp.minimum(i, ahead - 1)
                return (lax.rem(i, turns), lax.div(i, turns), 0, 0)

            def own(at):
                return pl.BlockSpec((slots, BLOCK, width), lambda i: (at, 0, 0), pipeline_mode=pl.Buffered(1))

            out_spec = pl.BlockSpec((slots, BLOCK, width), lambda i: (0, 0, 0))
            return pl.pallas_call(
                functools.partial(layer_kernel, devices=devices, head_dim=head_dim, heads=heads, layer=l, chunk_at=c * slots, gathers=gathers),
                grid=(ahead + q_tiles,),
                in_specs=[pl.BlockSpec((per, 1, BLOCK, width), turn), own(c)] + ([own(c + 1)] if gathers else []) + [any_spec] * 6
                + [whole(zero_b.shape)] + vectors + proj_specs(l, ahead) + bias_specs(l, ahead),
                out_specs=[out_spec] + ([any_spec] if gathers else []), out_shape=[row_shape] + ([full_shape] if gathers else []),
                scratch_shapes=attention_scratch(chunk) + [pltpu.VMEM((devices, slots, heads, head_dim, BLOCK), BF16), pltpu.VMEM((slots, BLOCK, cond_dim), BF16)]
                + row_scratch + [pltpu.SemaphoreType.DMA((6,)), pltpu.SemaphoreType.DMA((1,))] + exchange_sems(chunk) + gather_sems,
                compiler_params=params(collective_id=2 + c, has_side_effects=True), name='layer',
                cost_estimate=cost(chunk * attention_flops, heads * tokens * tokens * 2),
            )(x1, acts, *([x1s] if gathers else []), cond_rows, full_up, full_down, full_o, zero_t, ada_t, zero_b, ada_scale, ada_bias,
              w_proj, b_q_col, mask_row, pair_bias, pair_bias, pair_bias)

        def place(out, part, c):
            first_one = out is None
            return pl.pallas_call(
                place_kernel, grid=(slots,),
                in_specs=[pl.BlockSpec((devices, 1, BLOCK, width), lambda i: (0, i, 0, 0))] + ([] if first_one else [any_spec]),
                out_specs=pl.BlockSpec((1, devices, BLOCK, width), lambda i: (c * slots + i, 0, 0, 0)),
                out_shape=jax.ShapeDtypeStruct((all_slots, devices, BLOCK, width), BF16),
                input_output_aliases={} if first_one else {1: 0},
                compiler_params=params(), name='place',
            )(*((part,) if first_one else (part, out)))

        acts, x1s, full = rows_of_first(layer_start())
        parts = []
        for c in range(chunks):
            act, *rest = layer_of(full, acts, x1s, c)
            full = rest[0] if rest else None
            parts.append(lax.all_gather(act, 'tp'))
        out = None
        for c in range(chunks):
            out = place(out, parts[c], c)
        return out.reshape(samples, tokens, width)

    everywhere = P()
    in_specs = (P('dp', None, None), P('dp', None, None), P(None, 'tp', None, None), P(None), everywhere, everywhere, everywhere, everywhere, everywhere, P(None, None, None, 'tp'), P(None, 'tp'), P(None, 'tp', None), P(None, None, None, 'tp'), P(None, 'tp', None))
    return jax.shard_map(shard_body, mesh=mesh, in_specs=in_specs, out_specs=P('dp', None, None), check_vma=False)
```
